32 devices in a mesh: replica: 4 (over z), tp: 8 (over y, x, core).
Axes of the slice: x: 2, y: 2, z: 4, core: 2. Of those that a mesh axis runs over, the one named last changes fastest.
Arguments:
- hidden: bfloat16 [256, 8192], P(('replica', 'tp')), may hold values from -64 to 64
- head: bfloat16 [152064, 8192], P(('replica', 'tp'))
- token_ids: int32 [256], replicated, may hold values from 0 to 152063
Outputs:
- logprob: float32 [256], P(('replica', 'tp'))
The draws below stay inside these ranges and needn't reach their ends.
All inputs are finite; a program needn't handle non-finite values.
Results may differ from the reference program's by a relative error of at most 0.0003.
Values may be sent and summed in bfloat16 or wider, within the bound.
A program may use at most 128 MiB of HBM per device.

```python
import math
import jax
import jax.numpy as jnp
from jax import lax

D = 8192
V = 152064
SEQS = 256


def head_row(key, index):
    values = jax.random.normal(jax.random.fold_in(key, index), (D,), jnp.float32)
    return jnp.clip(values, -6.0, 6.0) * (3.0 / math.sqrt(D))


def head_rows(key, indices):
    base = jax.random.fold_in(key, 11)
    return jax.vmap(lambda index: head_row(base, index))(indices)


def draw_head(key, part):
    return head_rows(key, jnp.arange(V, dtype=jnp.int32)).astype(jnp.bfloat16)


def draw_hidden(key, part):
    drawn = jnp.clip(jax.random.normal(jax.random.fold_in(key, 21), (SEQS, D), jnp.float32), -6.0, 6.0)
    return drawn.astype(jnp.bfloat16)


def place_ends(result, rng, smallest, largest):
    index_at = [jax.random.randint(jax.random.fold_in(rng, axis), (), 0, length) for axis, length in enumerate(result.shape)]
    main_axis = result.shape.index(max(result.shape))
    beside = index_at[:main_axis] + [(index_at[main_axis] + 1) % result.shape[main_axis]] + index_at[main_axis + 1:]
    return result.at[tuple(index_at)].set(smallest).at[tuple(beside)].set(largest)


def setup_inputs(seed: int = 0) -> dict:
    key_list = jax.random.split(jax.random.key(seed), 4)
    return {
        "hidden": draw_hidden(jax.random.fold_in(key_list[3], 71), 0),
        "head": draw_head(jax.random.fold_in(key_list[3], 71), 0),
        "token_ids": place_ends(jax.random.randint(key_list[2], (SEQS,), 0, V), jax.random.fold_in(key_list[2], 1), 0, V - 1).astype(jnp.int32),
    }


def reference(hidden, head, token_ids):
    logits = lax.dot_general(hidden, head, (((1,), (1,)), ((), ())), preferred_element_type=jnp.float32)
    row_top = jnp.max(logits, axis=1)
    row_total = jnp.sum(jnp.exp(logits - row_top[:, None]), axis=1)
    row_picked = jnp.take_along_axis(logits, token_ids[:, None].astype(jnp.int32), axis=1)[:, 0]
    return row_picked - row_top - jnp.log(row_total)
```

```python
import functools

import jax
import jax.numpy as jnp
from jax import lax
from jax.experimental import pallas as pl
from jax.experimental.pallas import tpu as pltpu
from jax.sharding import PartitionSpec as P

MESH = pl.DeviceIdType.MESH
VMEM = 66_500_000
UNITS = 16
SINGLES = 4
PAIR = 2
LEAD = (4, 2)
COMM = True
COMPUTE = True


def chunk_rows(rows, limit):
    return max((r for r in range(16, limit + 1, 16) if rows % r == 0), default=rows)


def split_axis(size):
    return (size // 4, 2, 2) if size % 4 == 0 else (size, 1, 1)


def kernel(dims, unit, rows, tokens_ref, hidden_ref, head_ref, out_ref, ring, acc, gathered_a, gathered_b, hid,
           sent, arrived, ring_sem, own_sem, gsend, grecv, ssend, srecv):
    z_n, y_n, x_n, c_n = dims
    tp_n = y_n * x_n * c_n
    devices = z_n * tp_n
    z = lax.axis_index("replica")
    t = lax.axis_index("tp")
    me = z * tp_n + t
    y, x, c = t // (x_n * c_n), (t // c_n) % x_n, t % c_n
    at = (z, y, x, c)
    per_device, depth = hidden_ref.shape
    local_vocab = head_ref.shape[0]
    seqs = hid.shape[0]
    slots = ring.shape[0]
    gathered = (gathered_a, gathered_b)
    half = unit // 2

    def order(h):
        return (0, 1, 2, 3) if h % 2 == 0 else (0, 2, 1, 3)

    def columns(u, width=unit):
        return pl.ds(pl.multiple_of(u * unit, 128), width)

    def fetch(i):
        slot = i % slots
        return pltpu.make_async_copy(head_ref.at[:, columns(i * PAIR, PAIR * unit)], ring.at[slot], ring_sem.at[slot])

    def own(u, h):
        there = tuple(at[a] for a in reversed(order(h)))
        return pltpu.make_async_copy(
            hidden_ref.at[:, pl.ds(pl.multiple_of(u * unit + h * half, 128), half)],
            gathered[h].at[(u,) + there], own_sem.at[h])

    @pl.loop(0, UNITS)
    def _(u):
        own(u, 0).start()
        own(u, 1).start()

    @pl.loop(0, slots)
    def _(i):
        fetch(i).start()

    acc[...] = jnp.zeros_like(acc)

    def device(there):
        return (there[0], (there[1] * x_n + there[2]) * c_n + there[3])

    def peer(axis, k):
        there = list(at)
        there[axis] = (at[axis] + k) % dims[axis]
        return device(there)

    if COMM:
        barrier = pltpu.get_barrier_semaphore()
        for axis in range(4):
            for k in range(1, dims[axis]):
                pl.semaphore_signal(barrier, inc=1, device_id=peer(axis, k), device_id_type=MESH)
        pl.semaphore_wait(barrier, sum(dims) - 4)

    def remote(ref, h, phase, u, where):
        return pltpu.make_async_remote_copy(
            src_ref=ref, dst_ref=ref, send_sem=gsend.at[h, phase], recv_sem=grecv.at[u, h, phase],
            device_id=where, device_id_type=MESH)

    def block(u, h, phase):
        path = order(h)
        index = [slice(None) if a in path[:phase] else at[a] for a in reversed(path)]
        return gathered[h].at[(u,) + tuple(index)]

    def some(u, h, phase):
        count = dims[order(h)[phase]] - 1
        return gathered[h].at[(u,) + (0,) * (3 - phase) + (pl.ds(0, count),)]

    def hops(h, phase):
        return range(1, dims[order(h)[phase]])

    def arrive(u, h, phase):
        if dims[order(h)[phase]] > 1:
            remote(some(u, h, phase), h, phase, u, peer(3, 0)).wait_recv()

    def step(u, phase):
        if not COMM:
            return
        for h in (0, 1):
            if phase > 0:
                arrive(u, h, phase - 1)
            for k in hops(h, phase):
                remote(block(u, h, phase), h, phase, u, peer(order(h)[phase], k)).start()

    def finish(u):
        if COMM:
            for h in (0, 1):
                arrive(u, h, 3)
        for h in (0, 1):
            part = pl.ds(pl.multiple_of(u * unit + h * half, 128), half)
            for d in range(0, devices, 2):
                block = []
                for e in (d, d + 1):
                    there = (e // tp_n, e // (x_n * c_n) % y_n, e // c_n % x_n, e % c_n)
                    block.append(gathered[h][(u,) + tuple(there[a] for a in reversed(order(h)))].astype(jnp.float32))
                hid[d * per_device:(d + 2) * per_device, part] = jnp.concatenate(block, 0).astype(jnp.bfloat16)

    def product(u, low, count, width):
        spot = pl.ds(pl.multiple_of(u % PAIR * unit, 128), width)
        return lax.dot_general(ring[u // PAIR % slots, pl.ds(low, count), spot], hid[:, columns(u, width)],
                               (((1,), (1,)), ((), ())), preferred_element_type=jnp.float32)

    for h in (0, 1):
        there = tuple(at[a] for a in reversed(order(h)))
        mine = gathered[h].at[(slice(None),) + there]
        pltpu.make_async_copy(mine, mine, own_sem.at[h]).wait()

    @pl.loop(0, UNITS)
    def _(u):
        step(u, 0)

    first = [(u, 3) for u in range(2)] + [(u, 2) for u in range(2 + LEAD[1])] + [(u, 1) for u in range(2 + LEAD[0])]
    for u, phase in sorted(first, key=lambda e: (e[0] + 2 * e[1], e[1])):
        step(u, phase)

    def advance(u):
        for phase, lead in ((3, 0), (2, LEAD[1]), (1, LEAD[0])):
            @pl.when(u + lead < UNITS)
            def _():
                step(u + lead, phase)

    def ready(u, count):
        for v in range(count):
            finish(u + v)

        @pl.when(u % PAIR == 0)
        def _():
            fetch(u // PAIR).wait()

    def compute(u, count):
        ready(u, count)
        if COMPUTE:
            acc[...] += product(u, 0, local_vocab, count * unit)

        @pl.when(((u + count) % PAIR == 0) & (u // PAIR + slots < UNITS // PAIR))
        def _():
            fetch(u // PAIR + slots).start()

    @pl.loop(0, SINGLES)
    def _(u):
        @pl.when(u > 0)
        def _():
            advance(u + 1 + u // (SINGLES - 1))

        @pl.when(u == SINGLES - 2)
        def _():
            advance(u + 2)
        compute(u, 1)

    pairs = (UNITS - SINGLES) // PAIR - 1

    @pl.loop(0, pairs)
    def _(i):
        for v in range(PAIR):
            advance(SINGLES + (i + 1) * PAIR + v)
        compute(SINGLES + i * PAIR, PAIR)

    final = UNITS - PAIR
    ready(final, PAIR)
    tokens = tokens_ref[...] - me * local_vocab
    blocks = local_vocab // rows
    inner = 3 if blocks % 3 == 0 else 1

    big = rows * inner

    def measure(i, carry):
        top, total, picked = carry
        for b in range(inner):
            low = pl.multiple_of(i * big + b * rows, 8)
            logits = acc[pl.ds(low, rows), :]
            new_top = jnp.maximum(top, jnp.max(logits, axis=0, keepdims=True))
            line = lax.broadcasted_iota(jnp.int32, logits.shape, 0)
            picked += jnp.sum(jnp.where(line == tokens - low, logits, 0.0), axis=0, keepdims=True)
            total = total * jnp.exp(top - new_top) + jnp.sum(jnp.exp(logits - new_top), axis=0, keepdims=True)
            top = new_top
        return top, total, picked

    def finalize(i):
        low = pl.multiple_of(i * big, 8)
        acc[pl.ds(low, big), :] += product(final, low, big, PAIR * unit)

    def close(i, carry):
        carry = measure(i - 1, carry)
        finalize(i)
        return carry

    carry = (jnp.full((1, seqs), -jnp.inf, jnp.float32),) + (jnp.zeros((1, seqs), jnp.float32),) * 2
    finalize(0)
    carry = lax.fori_loop(1, blocks // inner, close, carry)
    top, total, picked = measure(blocks // inner - 1, carry)

    groups, _, _, lanes = sent.shape
    for g in range(groups):
        part = slice(g * lanes, (g + 1) * lanes)
        sent[g, 0, 0:1, :] = top[:, part]
        sent[g, 0, 1:2, :] = picked[:, part]
        sent[g, 1, :, :] = jnp.broadcast_to(total[:, part], (2, lanes))
    apart = lanes // per_device

    if COMM:
        arrived[pl.ds(me, 1)] = sent[pl.ds(me // apart, 1)]

    def result(k):
        d = (me + k) % devices
        return pltpu.make_async_remote_copy(
            src_ref=sent.at[d // apart], dst_ref=arrived.at[me], send_sem=ssend, recv_sem=srecv,
            device_id=(d // tp_n, d % tp_n), device_id_type=MESH)

    if COMM:
        @pl.loop(1, devices)
        def _(k):
            result(k).start()

        for h in (0, 1):
            for phase in range(4):
                if dims[order(h)[phase]] > 1:
                    remote(some(slice(None), h, phase), h, phase, 0, peer(3, 0)).wait_send()

        if devices > 1:
            everyone = pltpu.make_async_remote_copy(
                src_ref=arrived.at[pl.ds(0, devices - 1)], dst_ref=arrived.at[pl.ds(0, devices - 1)],
                send_sem=ssend, recv_sem=srecv, device_id=peer(3, 0), device_id_type=MESH)
            everyone.wait_recv()
            everyone.wait_send()

    firsts, totals = arrived[:, 0], arrived[:, 1]
    top = jnp.max(firsts, axis=0)
    total = jnp.sum(totals * jnp.exp(firsts - top), axis=0)
    picked = jnp.sum(firsts, axis=0)
    value = picked[1:2] - top[0:1] - jnp.log(total[0:1])
    lane = lax.broadcasted_iota(jnp.int32, (per_device, lanes), 1)
    row = lax.broadcasted_iota(jnp.int32, (per_device, lanes), 0) + (me % apart) * per_device
    mine = jnp.sum(jnp.where(lane == row, value, 0.0), axis=1, keepdims=True)
    out_ref[...] = jnp.broadcast_to(mine, out_ref.shape)


def shards(z_n, tp_n, hidden, head, token_ids):
    dims = (z_n,) + split_axis(tp_n)
    devices = z_n * tp_n
    per_device, depth = hidden.shape
    local_vocab = head.shape[0]
    seqs = per_device * devices
    rows = chunk_rows(local_vocab, 528)
    unit = depth // UNITS
    fixed = local_vocab * seqs * 4 + 2 * seqs * depth * 2 + 3 * 2**20
    wide = PAIR * unit
    slots = min(depth // wide, (VMEM - fixed - local_vocab * seqs * 5) // (local_vocab * wide * 2))
    stores = [tuple(dims[a] for a in reversed(path)) for path in ((0, 1, 2, 3), (0, 2, 1, 3))]
    lanes = 128
    out = pl.pallas_call(
        functools.partial(kernel, dims, unit, rows),
        out_shape=jax.ShapeDtypeStruct((per_device, 128), jnp.float32),
        in_specs=[pl.BlockSpec(memory_space=pltpu.VMEM), pl.BlockSpec(memory_space=pltpu.HBM),
                  pl.BlockSpec(memory_space=pltpu.HBM)],
        out_specs=pl.BlockSpec(memory_space=pltpu.VMEM),
        scratch_shapes=[
            pltpu.VMEM((slots, local_vocab, wide), jnp.bfloat16),
            pltpu.VMEM((local_vocab, seqs), jnp.float32),
            pltpu.VMEM((UNITS,) + stores[0] + (per_device, unit // 2), jnp.bfloat16),
            pltpu.VMEM((UNITS,) + stores[1] + (per_device, unit // 2), jnp.bfloat16),
            pltpu.VMEM((seqs, depth), jnp.bfloat16),
            pltpu.VMEM((seqs // lanes, 2, 2, lanes), jnp.float32),
            pltpu.VMEM((devices, 2, 2, lanes), jnp.float32),
            pltpu.SemaphoreType.DMA((slots,)),
            pltpu.SemaphoreType.DMA((2,)),
            pltpu.SemaphoreType.DMA((2, 4)),
            pltpu.SemaphoreType.DMA((UNITS, 2, 4)),
            pltpu.SemaphoreType.DMA,
            pltpu.SemaphoreType.DMA,
        ],
        compiler_params=pltpu.CompilerParams(
            has_side_effects=True, vmem_limit_bytes=67_000_000, **(dict(collective_id=0) if COMM else {})),
    )(token_ids.reshape(1, seqs), hidden, head)
    return out[:, 0]


def solution(mesh):
    in_specs = (P(("replica", "tp"), None), P(("replica", "tp"), None), P())
    body = functools.partial(shards, mesh.shape["replica"], mesh.shape["tp"])
    return jax.shard_map(body, mesh=mesh, in_specs=in_specs, out_specs=P(("replica", "tp")), check_vma=False)
```

```python
import functools

import jax
import jax.numpy as jnp
from jax import lax
from jax.experimental import pallas as pl
from jax.experimental.pallas import tpu as pltpu
from jax.sharding import PartitionSpec as P

MESH = pl.DeviceIdType.MESH
VMEM = 66_500_000
UNITS = 16
SINGLES = 4
PAIR = 2
LEAD = (5, 2)
COMM = True
COMPUTE = True


def chunk_rows(rows, limit):
    return max((r for r in range(16, limit + 1, 16) if rows % r == 0), default=rows)


def split_axis(size):
    return (size // 4, 2, 2) if size % 4 == 0 else (size, 1, 1)


def kernel(dims, unit, rows, tokens_ref, hidden_ref, head_ref, out_ref, ring, acc, gathered_a, gathered_b, hid,
           sent, arrived, ring_sem, own_sem, gsend, grecv, ssend, srecv):
    z_n, y_n, x_n, c_n = dims
    tp_n = y_n * x_n * c_n
    devices = z_n * tp_n
    z = lax.axis_index("replica")
    t = lax.axis_index("tp")
    me = z * tp_n + t
    y, x, c = t // (x_n * c_n), (t // c_n) % x_n, t % c_n
    at = (z, y, x, c)
    per_device, depth = hidden_ref.shape
    local_vocab = head_ref.shape[0]
    seqs = hid.shape[0]
    slots = ring.shape[0]
    gathered = (gathered_a, gathered_b)
    half = unit // 2

    def order(h):
        return (0, 1, 2, 3) if h % 2 == 0 else (0, 2, 1, 3)

    def columns(u, width=unit):
        return pl.ds(pl.multiple_of(u * unit, 128), width)

    def fetch(i):
        slot = i % slots
        return pltpu.make_async_copy(head_ref.at[:, columns(i * PAIR, PAIR * unit)], ring.at[slot], ring_sem.at[slot])

    def own(u, h):
        there = tuple(at[a] for a in reversed(order(h)))
        return pltpu.make_async_copy(
            hidden_ref.at[:, pl.ds(pl.multiple_of(u * unit + h * half, 128), half)],
            gathered[h].at[(u,) + there], own_sem.at[h])

    @pl.loop(0, UNITS)
    def _(u):
        own(u, 0).start()
        own(u, 1).start()

    @pl.loop(0, slots)
    def _(i):
        fetch(i).start()

    acc[...] = jnp.zeros_like(acc)

    def device(there):
        return (there[0], (there[1] * x_n + there[2]) * c_n + there[3])

    def peer(axis, k):
        there = list(at)
        there[axis] = (at[axis] + k) % dims[axis]
        return device(there)

    if COMM:
        barrier = pltpu.get_barrier_semaphore()
        for axis in range(4):
            for k in range(1, dims[axis]):
                pl.semaphore_signal(barrier, inc=1, device_id=peer(axis, k), device_id_type=MESH)
        pl.semaphore_wait(barrier, sum(dims) - 4)

    def remote(ref, h, phase, u, where):
        return pltpu.make_async_remote_copy(
            src_ref=ref, dst_ref=ref, send_sem=gsend.at[h, phase], recv_sem=grecv.at[u, h, phase],
            device_id=where, device_id_type=MESH)

    def block(u, h, phase):
        path = order(h)
        index = [slice(None) if a in path[:phase] else at[a] for a in reversed(path)]
        return gathered[h].at[(u,) + tuple(index)]

    def some(u, h, phase):
        count = dims[order(h)[phase]] - 1
        return gathered[h].at[(u,) + (0,) * (3 - phase) + (pl.ds(0, count),)]

    def hops(h, phase):
        return range(1, dims[order(h)[phase]])

    def arrive(u, h, phase):
        if dims[order(h)[phase]] > 1:
            remote(some(u, h, phase), h, phase, u, peer(3, 0)).wait_recv()

    def step(u, phase):
        if not COMM:
            return
        for h in (0, 1):
            if phase > 0:
                arrive(u, h, phase - 1)
            for k in hops(h, phase):
                remote(block(u, h, phase), h, phase, u, peer(order(h)[phase], k)).start()

    def finish(u):
        if COMM:
            for h in (0, 1):
                arrive(u, h, 3)
        for h in (0, 1):
            part = pl.ds(pl.multiple_of(u * unit + h * half, 128), half)
            for d in range(0, devices, 2):
                block = []
                for e in (d, d + 1):
                    there = (e // tp_n, e // (x_n * c_n) % y_n, e // c_n % x_n, e % c_n)
                    block.append(gathered[h][(u,) + tuple(there[a] for a in reversed(order(h)))].astype(jnp.float32))
                hid[d * per_device:(d + 2) * per_device, part] = jnp.concatenate(block, 0).astype(jnp.bfloat16)

    def product(u, low, count, width):
        spot = pl.ds(pl.multiple_of(u % PAIR * unit, 128), width)
        return lax.dot_general(ring[u // PAIR % slots, pl.ds(low, count), spot], hid[:, columns(u, width)],
                               (((1,), (1,)), ((), ())), preferred_element_type=jnp.float32)

    for h in (0, 1):
        there = tuple(at[a] for a in reversed(order(h)))
        mine = gathered[h].at[(slice(None),) + there]
        pltpu.make_async_copy(mine, mine, own_sem.at[h]).wait()

    @pl.loop(0, UNITS)
    def _(u):
        step(u, 0)

    first = [(u, 3) for u in range(2)] + [(u, 2) for u in range(2 + LEAD[1])] + [(u, 1) for u in range(2 + LEAD[0])]
    for u, phase in sorted(first, key=lambda e: (e[0] + 2 * e[1], e[1])):
        step(u, phase)

    def advance(u):
        for phase, lead in ((3, 0), (2, LEAD[1]), (1, LEAD[0])):
            @pl.when(u + lead < UNITS)
            def _():
                step(u + lead, phase)

    def ready(u, count):
        for v in range(count):
            finish(u + v)

        @pl.when(u % PAIR == 0)
        def _():
            fetch(u // PAIR).wait()

    def compute(u, count):
        ready(u, count)
        if COMPUTE:
            acc[...] += product(u, 0, local_vocab, count * unit)

        @pl.when(((u + count) % PAIR == 0) & (u // PAIR + slots < UNITS // PAIR))
        def _():
            fetch(u // PAIR + slots).start()

    @pl.loop(0, SINGLES)
    def _(u):
        @pl.when(u > 0)
        def _():
            advance(u + 1 + u // (SINGLES - 1))

        @pl.when(u == SINGLES - 2)
        def _():
            advance(u + 2)
        compute(u, 1)

    pairs = (UNITS - SINGLES) // PAIR - 1

    @pl.loop(0, pairs)
    def _(i):
        for v in range(PAIR):
            advance(SINGLES + (i + 1) * PAIR + v)
        compute(SINGLES + i * PAIR, PAIR)

    final = UNITS - PAIR
    ready(final, PAIR)
    tokens = tokens_ref[...] - me * local_vocab
    top = jnp.full((1, seqs), -jnp.inf, jnp.float32)
    picked = jnp.zeros((1, seqs), jnp.float32)
    for low in range(0, local_vocab, rows):
        logits = acc[low:low + rows, :] + product(final, low, rows, PAIR * unit)
        acc[low:low + rows, :] = logits
        line = lax.broadcasted_iota(jnp.int32, logits.shape, 0)
        picked += jnp.sum(jnp.where(line == tokens - low, logits, 0.0), axis=0, keepdims=True)
        top = jnp.maximum(top, jnp.max(logits, axis=0, keepdims=True))

    def add(i, total):
        part = acc[pl.ds(pl.multiple_of(i * rows, 8), rows), :]
        return total + jnp.sum(jnp.exp(part - top), axis=0, keepdims=True)

    total = lax.fori_loop(0, local_vocab // rows, add, jnp.zeros((1, seqs), jnp.float32))

    groups, _, _, lanes = sent.shape
    for g in range(groups):
        part = slice(g * lanes, (g + 1) * lanes)
        sent[g, 0, 0:1, :] = top[:, part]
        sent[g, 0, 1:2, :] = picked[:, part]
        sent[g, 1, :, :] = jnp.broadcast_to(total[:, part], (2, lanes))
    apart = lanes // per_device

    if COMM:
        arrived[pl.ds(me, 1)] = sent[pl.ds(me // apart, 1)]

    def result(k):
        d = (me + k) % devices
        return pltpu.make_async_remote_copy(
            src_ref=sent.at[d // apart], dst_ref=arrived.at[me], send_sem=ssend, recv_sem=srecv,
            device_id=(d // tp_n, d % tp_n), device_id_type=MESH)

    if COMM:
        @pl.loop(1, devices)
        def _(k):
            result(k).start()

        for h in (0, 1):
            for phase in range(4):
                if dims[order(h)[phase]] > 1:
                    remote(some(slice(None), h, phase), h, phase, 0, peer(3, 0)).wait_send()

        if devices > 1:
            everyone = pltpu.make_async_remote_copy(
                src_ref=arrived.at[pl.ds(0, devices - 1)], dst_ref=arrived.at[pl.ds(0, devices - 1)],
                send_sem=ssend, recv_sem=srecv, device_id=peer(3, 0), device_id_type=MESH)
            everyone.wait_recv()
            everyone.wait_send()

    firsts, totals = arrived[:, 0], arrived[:, 1]
    top = jnp.max(firsts, axis=0)
    total = jnp.sum(totals * jnp.exp(firsts - top), axis=0)
    picked = jnp.sum(firsts, axis=0)
    value = picked[1:2] - top[0:1] - jnp.log(total[0:1])
    lane = lax.broadcasted_iota(jnp.int32, (per_device, lanes), 1)
    row = lax.broadcasted_iota(jnp.int32, (per_device, lanes), 0) + (me % apart) * per_device
    mine = jnp.sum(jnp.where(lane == row, value, 0.0), axis=1, keepdims=True)
    out_ref[...] = jnp.broadcast_to(mine, out_ref.shape)


def shards(z_n, tp_n, hidden, head, token_ids):
    dims = (z_n,) + split_axis(tp_n)
    devices = z_n * tp_n
    per_device, depth = hidden.shape
    local_vocab = head.shape[0]
    seqs = per_device * devices
    rows = chunk_rows(local_vocab, 1584)
    unit = depth // UNITS
    fixed = local_vocab * seqs * 4 + 2 * seqs * depth * 2 + 3 * 2**20
    wide = PAIR * unit
    slots = min(3, depth // wide, (VMEM - fixed - local_vocab * seqs * 5) // (local_vocab * wide * 2))
    stores = [tuple(dims[a] for a in reversed(path)) for path in ((0, 1, 2, 3), (0, 2, 1, 3))]
    lanes = 128
    out = pl.pallas_call(
        functools.partial(kernel, dims, unit, rows),
        out_shape=jax.ShapeDtypeStruct((per_device, 128), jnp.float32),
        in_specs=[pl.BlockSpec(memory_space=pltpu.VMEM), pl.BlockSpec(memory_space=pltpu.HBM),
                  pl.BlockSpec(memory_space=pltpu.HBM)],
        out_specs=pl.BlockSpec(memory_space=pltpu.VMEM),
        scratch_shapes=[
            pltpu.VMEM((slots, local_vocab, wide), jnp.bfloat16),
            pltpu.VMEM((local_vocab, seqs), jnp.float32),
            pltpu.VMEM((UNITS,) + stores[0] + (per_device, unit // 2), jnp.bfloat16),
            pltpu.VMEM((UNITS,) + stores[1] + (per_device, unit // 2), jnp.bfloat16),
            pltpu.VMEM((seqs, depth), jnp.bfloat16),
            pltpu.VMEM((seqs // lanes, 2, 2, lanes), jnp.float32),
            pltpu.VMEM((devices, 2, 2, lanes), jnp.float32),
            pltpu.SemaphoreType.DMA((slots,)),
            pltpu.SemaphoreType.DMA((2,)),
            pltpu.SemaphoreType.DMA((2, 4)),
            pltpu.SemaphoreType.DMA((UNITS, 2, 4)),
            pltpu.SemaphoreType.DMA,
            pltpu.SemaphoreType.DMA,
        ],
        compiler_params=pltpu.CompilerParams(
            has_side_effects=True, vmem_limit_bytes=67_000_000, **(dict(collective_id=0) if COMM else {})),
    )(token_ids.reshape(1, seqs), hidden, head)
    return out[:, 0]


def solution(mesh):
    in_specs = (P(("replica", "tp"), None), P(("replica", "tp"), None), P())
    body = functools.partial(shards, mesh.shape["replica"], mesh.shape["tp"])
    return jax.shard_map(body, mesh=mesh, in_specs=in_specs, out_specs=P(("replica", "tp")), check_vma=False)
```
